32 devices in a mesh: coef: 2 (over y), grid: 16 (over z, x, core).
Axes of the slice: x: 2, y: 2, z: 4, core: 2. Of those that a mesh axis runs over, the one named last changes fastest.
Arguments:
- basis_values: bfloat16 [10240, 2688], P('grid'), may hold values from -6 to 6
- occ_coef: bfloat16 [10240, 1024], P('grid', 'coef'), may hold values from -0.125 to 0.125
- listed_panels: int32 [16, 21], P('grid'), may hold values from 0 to 79, as said below
- centres: float32 [3, 10240], replicated, may hold values from 0 to 4
- point_weights: float32 [10240], P('grid'), may hold values from 0.25 to 4
Outputs:
- exchange_tiles: float32 [10240, 1024], P('grid', 'coef')
The draws below stay inside these ranges and needn't reach their ends.
Inputs may be any that keep to these rules, and one draw needn't show every extreme that they name: `listed_panels`: the panels of one batch are distinct; panel p belongs to batch p // 5, and batch b names only panels of batches b - 4 to b + 4.
All inputs are finite; a program needn't handle non-finite values.
Results may differ from the reference program's by a relative error of at most 0.0085.
Values may be sent and summed in bfloat16 or wider, within the bound.
No kernel may reach another device: no remote copies, remote signals or barrier semaphores. Data moves between devices by JAX's collectives and lax.ppermute only.
A program may use at most 64 MiB of HBM per device.

```python
import math
import jax
import jax.numpy as jnp
from jax import lax

ORBITALS = 1024
PANEL_ROWS = 128
PANELS_DEV = 5
REACH = 4
LISTED = 21
POINTS_DEV = 640
PANELS = 80
FUNCTIONS = 10240
POINTS = 10240
N_COEF = 2
N_GRID = 16


def draw_listed_panels(key, part):
    batches = jnp.arange(N_GRID, dtype=jnp.int32)
    slots = jnp.arange((2 * REACH + 1) * PANELS_DEV, dtype=jnp.int32)
    candidates = (batches[:, None] - REACH) * PANELS_DEV + slots[None, :]
    valid = (candidates >= 0) & (candidates < PANELS)
    noise = jax.random.randint(key, candidates.shape, 0, 2 ** 20, dtype=jnp.int32)
    scores = jnp.where(valid, noise * 64 + slots[None, :], -1)
    picked = lax.top_k(scores, LISTED)[1]
    return jnp.take_along_axis(candidates, picked, axis=1).astype(jnp.int32)


def block_levels(own_key, dims, cuts, least, largest):
    factor_of, own = 1.0, jax.random.fold_in(own_key, 6)
    for dim, parts in cuts:
        steps = jnp.exp(jax.random.uniform(jax.random.fold_in(own, dim), (parts,), jnp.float32, least / len(cuts), largest / len(cuts)))
        factor_of = factor_of * jnp.repeat(steps, dims[dim] // parts).reshape([-1 if axis == dim else 1 for axis in range(len(dims))])
    return factor_of


def centred(own_key, dims, spread, most, split=(), kind=jnp.bfloat16):
    gain = block_levels(own_key, dims, split, -0.22, 0.18) if split else 1.0
    values = jax.random.normal(own_key, dims, jnp.float32) * spread * gain
    return jnp.minimum(jnp.maximum(values, -most), most).astype(kind)


def setup_inputs(seed: int = 0) -> dict:
    seeds = jax.random.split(jax.random.key(seed), 6)
    return {
        "basis_values": centred(seeds[0], (POINTS, LISTED * PANEL_ROWS), 1.0, 6.0, ((0, 16),)),
        "occ_coef": centred(seeds[1], (FUNCTIONS, ORBITALS), (LISTED * PANEL_ROWS) ** -0.5, 0.125, ((0, 16), (1, 2))),
        "listed_panels": draw_listed_panels(jax.random.fold_in(seeds[5], 71), 0),
        "centres": jnp.clip(jax.random.uniform(seeds[3], (3, POINTS), jnp.float32, 0.0, 4.0), 0.0, 4.0),
        "point_weights": jnp.clip(jnp.exp(math.log(4.0) - 2.7725887 * jax.random.uniform(seeds[4], (POINTS,), jnp.float32) ** block_levels(seeds[4], (POINTS,), ((0, 16),), -0.2, 0.2)), 0.25, 4.0),
    }


def reference(basis_values, occ_coef, listed_panels, centres, point_weights):
    panels = occ_coef.reshape(PANELS, PANEL_ROWS, ORBITALS)
    block = ORBITALS // N_COEF
    anchor = jnp.zeros((), jnp.int32)

    def orbital_field(batch):
        start = (batch * POINTS_DEV).astype(jnp.int32)
        rows = lax.dynamic_slice_in_dim(basis_values, start, POINTS_DEV, 0)
        chosen = jnp.take(panels, listed_panels[batch], axis=0).reshape(LISTED * PANEL_ROWS, ORBITALS)
        return jnp.dot(rows, chosen, preferred_element_type=jnp.float32).astype(jnp.bfloat16)
    fields = lax.map(orbital_field, jnp.arange(N_GRID, dtype=jnp.int32))
    zeros = jnp.zeros((1, POINTS_DEV, ORBITALS), jnp.bfloat16)
    padded = jnp.concatenate([zeros, fields, zeros], 0)
    padded_centres = jnp.pad(centres, ((0, 0), (POINTS_DEV, POINTS_DEV)))

    def step(total, batch):
        start = (batch * POINTS_DEV).astype(jnp.int32)
        own = padded[batch + 1]
        near = lax.dynamic_slice_in_dim(padded, batch.astype(jnp.int32), 3, 0).reshape(3 * POINTS_DEV, ORBITALS)
        density = jnp.zeros((POINTS_DEV, 3 * POINTS_DEV), jnp.float32)
        for part in range(N_COEF):
            left = own[:, part * block:(part + 1) * block]
            right = near[:, part * block:(part + 1) * block]
            term = lax.dot_general(left, right, (((1,), (1,)), ((), ())), preferred_element_type=jnp.float32)
            term = lax.optimization_barrier((term / jnp.sqrt(jnp.float32(ORBITALS))).astype(jnp.bfloat16))
            density = density + term.astype(jnp.float32)
        own_centres = lax.dynamic_slice(centres, (anchor, start), (3, POINTS_DEV))
        near_centres = lax.dynamic_slice(padded_centres, (anchor, start), (3, 3 * POINTS_DEV))
        distance = jnp.zeros((POINTS_DEV, 3 * POINTS_DEV), jnp.float32)
        for axis in range(3):
            gap = own_centres[axis][:, None] - near_centres[axis][None, :]
            distance = distance + gap * gap
        kernel = 1.0 / jnp.sqrt(distance + 0.25)
        mixed = (kernel * density).astype(jnp.bfloat16)
        exchanged = jnp.dot(mixed, near, preferred_element_type=jnp.float32)
        weights = lax.dynamic_slice_in_dim(point_weights, start, POINTS_DEV, 0)
        weighted = (exchanged * weights[:, None] / jnp.sqrt(jnp.float32(3 * POINTS_DEV))).astype(jnp.bfloat16)
        rows = lax.dynamic_slice_in_dim(basis_values, start, POINTS_DEV, 0)
        tiles = lax.dot_general(rows, weighted, (((0,), (0,)), ((), ())), preferred_element_type=jnp.float32)
        tiles = tiles / jnp.sqrt(jnp.float32(POINTS_DEV))
        total = total.at[listed_panels[batch]].add(tiles.reshape(LISTED, PANEL_ROWS, ORBITALS))
        return (total, None)
    begin = jnp.zeros((PANELS, PANEL_ROWS, ORBITALS), jnp.float32)
    total, unused = lax.scan(step, begin, jnp.arange(N_GRID, dtype=jnp.int32))
    return total.reshape(FUNCTIONS, ORBITALS)
```

```python
import functools
import jax
import jax.numpy as jnp
from jax import lax
from jax.experimental import pallas as pl
from jax.experimental.pallas import tpu as pltpu
from jax.sharding import PartitionSpec as P

ORBITALS = 1024
PANEL_ROWS = 128
PANELS_DEV = 5
REACH = 4
LISTED = 21
CHUNKS = 2
LANES = 128


def from_behind(block, distance):
    devices = range(lax.axis_size("grid"))
    route = [(i - distance, i) for i in devices if i - distance in devices]
    return lax.ppermute(block, "grid", route)


def core_swap(block):
    return lax.ppermute(block, "grid", [(i, i ^ 1) for i in range(lax.axis_size("grid"))])


def outer_halo(block):
    count = lax.axis_size("grid")
    route = []
    for i in range(1, count - 1, 2):
        route += [(i, i + 1), (i + 1, i)]
    return lax.ppermute(block, "grid", route)


def coef_shift(block, shift):
    count = lax.axis_size("coef")
    return lax.ppermute(block, "coef", [(i, (i + shift) % count) for i in range(count)])


VMEM = pl.BlockSpec(memory_space=pltpu.VMEM)
ANY = pl.BlockSpec(memory_space=pl.ANY)


def field_body(table, basis, *refs):
    blocks, out, chosen, sems = refs[:-3], refs[-3], refs[-2], refs[-1]

    def start(s, carry):
        block, row = table[0, s], pl.multiple_of(table[1, s] * PANEL_ROWS, PANEL_ROWS)
        target = chosen.at[pl.ds(pl.multiple_of(s * PANEL_ROWS, PANEL_ROWS), PANEL_ROWS)]
        for j, ref in enumerate(blocks):
            @pl.when(block == j)
            def _():
                pltpu.make_async_copy(ref.at[pl.ds(row, PANEL_ROWS)], target, sems.at[s]).start()
        return carry

    def wait(s, carry):
        target = chosen.at[pl.ds(pl.multiple_of(s * PANEL_ROWS, PANEL_ROWS), PANEL_ROWS)]
        pltpu.make_async_copy(blocks[0].at[pl.ds(0, PANEL_ROWS)], target, sems.at[s]).wait()
        return carry

    lax.fori_loop(0, LISTED, start, 0)
    lax.fori_loop(0, LISTED, wait, 0)
    out[...] = jnp.dot(basis[...], chosen[...], preferred_element_type=jnp.float32).astype(out.dtype)


def field_of(table, basis, blocks):
    points, width = basis.shape[0], blocks[0].shape[1]
    return pl.pallas_call(
        field_body,
        out_shape=jax.ShapeDtypeStruct((points, width), jnp.bfloat16),
        in_specs=[pl.BlockSpec(memory_space=pltpu.SMEM), VMEM] + [ANY] * len(blocks),
        out_specs=VMEM,
        scratch_shapes=[
            pltpu.VMEM((LISTED * PANEL_ROWS, width), jnp.bfloat16),
            pltpu.SemaphoreType.DMA((LISTED,)),
        ],
        cost_estimate=pl.CostEstimate(
            flops=2 * basis.size * width, bytes_accessed=4 * basis.size, transcendentals=0
        ),
        name="field",
    )(table, basis, *blocks)


def mixed_body(terms, chunks, rows, own_centres, near_centres, *refs):
    fields, out = refs[:-1], refs[-1]
    points = fields[0].shape[0]
    here = pl.ds(pl.multiple_of(pl.program_id(0) * rows, rows), rows)
    scale = 1.0 / float(ORBITALS) ** 0.5
    for near in range(3):
        density = jnp.zeros((rows, points), jnp.float32)
        for term in range(terms):
            total = jnp.zeros((rows, points), jnp.float32)
            for chunk in range(chunks):
                at = term * chunks + chunk
                total = total + lax.dot_general(
                    fields[at][here, :],
                    fields[near * terms * chunks + at][...],
                    (((1,), (1,)), ((), ())),
                    preferred_element_type=jnp.float32,
                )
            density = density + (total * scale).astype(jnp.bfloat16).astype(jnp.float32)
        distance = jnp.zeros((rows, points), jnp.float32)
        for axis in range(3):
            gap = own_centres[here, axis : axis + 1] - near_centres[
                axis : axis + 1, near * points : (near + 1) * points
            ]
            distance = distance + gap * gap
        out[:, near * points : (near + 1) * points] = (
            lax.rsqrt(distance + 0.25) * density
        ).astype(out.dtype)


def mixed_of(own_centres, near_centres, fields, terms, chunks):
    points = own_centres.shape[0]
    rows = points // 2 if points % 32 == 0 else points
    width = fields[0].shape[1]
    return pl.pallas_call(
        functools.partial(mixed_body, terms, chunks, rows),
        grid=(points // rows,),
        out_shape=jax.ShapeDtypeStruct((points, 3 * points), jnp.bfloat16),
        in_specs=[VMEM] * (2 + len(fields)),
        out_specs=pl.BlockSpec((rows, 3 * points), lambda i: (i, 0)),
        cost_estimate=pl.CostEstimate(
            flops=6 * points * points * width * chunks * terms,
            bytes_accessed=16 * points * points,
            transcendentals=3 * points * points,
        ),
        name="mixed",
    )(own_centres, near_centres, *fields)


def tiles_body(table, mixed, own, swapped, outer, weights, turned, stay, leave, tiles):
    points = own.shape[0]
    exchanged = jnp.dot(mixed[:, :points], own[...], preferred_element_type=jnp.float32)
    exchanged += jnp.dot(
        mixed[:, points : 2 * points], swapped[...], preferred_element_type=jnp.float32
    )
    exchanged += jnp.dot(mixed[:, 2 * points :], outer[...], preferred_element_type=jnp.float32)
    weighted = (exchanged * weights[...] / jnp.sqrt(jnp.float32(3 * points))).astype(jnp.bfloat16)
    product = jnp.dot(turned[...], weighted, preferred_element_type=jnp.float32)
    tiles[...] = (product / jnp.sqrt(jnp.float32(points))).astype(tiles.dtype)
    stay[...] = jnp.zeros(stay.shape, stay.dtype)
    leave[...] = jnp.zeros(leave.shape, leave.dtype)
    blocks = stay.shape[0] // (PANELS_DEV * PANEL_ROWS)

    def place(s, carry):
        block, panel = table[0, s], table[1, s]
        tile = tiles[pl.ds(pl.multiple_of(s * PANEL_ROWS, PANEL_ROWS), PANEL_ROWS), :]
        row = block * PANELS_DEV + panel

        @pl.when(block < blocks)
        def _():
            stay[pl.ds(pl.multiple_of(row * PANEL_ROWS, PANEL_ROWS), PANEL_ROWS), :] = tile

        @pl.when(block >= blocks)
        def _():
            far = row - blocks * PANELS_DEV
            leave[pl.ds(pl.multiple_of(far * PANEL_ROWS, PANEL_ROWS), PANEL_ROWS), :] = tile

        return carry

    lax.fori_loop(0, LISTED, place, 0)


def tiles_of(table, mixed, own, swapped, outer, weights, turned):
    width = own.shape[1]
    block = PANELS_DEV * PANEL_ROWS
    return pl.pallas_call(
        tiles_body,
        out_shape=(
            jax.ShapeDtypeStruct(((REACH + 1) * block, width), jnp.bfloat16),
            jax.ShapeDtypeStruct((REACH * block, width), jnp.bfloat16),
        ),
        in_specs=[pl.BlockSpec(memory_space=pltpu.SMEM)] + [VMEM] * 6,
        out_specs=(VMEM, VMEM),
        scratch_shapes=[pltpu.VMEM((LISTED * PANEL_ROWS, width), jnp.bfloat16)],
        cost_estimate=pl.CostEstimate(
            flops=2 * (mixed.size + turned.size) * width,
            bytes_accessed=4 * turned.size,
            transcendentals=0,
        ),
        name="tiles",
    )(table, mixed, own, swapped, outer, weights, turned)


def paired_body(core, stay, came, *outs):
    block = PANELS_DEV * PANEL_ROWS
    middle = REACH // 2
    for i, out in enumerate(outs):
        own = stay[i * block : (i + 1) * block, :].astype(jnp.float32)
        if i in (0, REACH):
            far = came[(REACH - 1) * block : REACH * block, :].astype(jnp.float32)
            mine = core[0] == (1 if i == 0 else 0)
            total = own + jnp.where(mine, far, 0.0)
        else:
            total = own + came[(i - 1) * block : i * block, :].astype(jnp.float32)
        out[...] = total.astype(out.dtype)


def paired_of(core, stay, came):
    block, width = PANELS_DEV * PANEL_ROWS, stay.shape[1]
    kinds = [jnp.float32 if i == REACH // 2 else jnp.bfloat16 for i in range(REACH + 1)]
    return pl.pallas_call(
        paired_body,
        out_shape=tuple(jax.ShapeDtypeStruct((block, width), kind) for kind in kinds),
        in_specs=[pl.BlockSpec(memory_space=pltpu.SMEM), VMEM, VMEM],
        out_specs=(VMEM,) * len(kinds),
        cost_estimate=pl.CostEstimate(
            flops=2 * stay.size, bytes_accessed=6 * stay.size, transcendentals=0
        ),
        name="paired",
    )(core, stay, came)


def total_body(chunks, *refs):
    out = refs[-1]
    width = out.shape[1] // chunks
    each = (len(refs) - 1) // chunks
    for chunk in range(chunks):
        total = refs[chunk * each][...]
        for ref in refs[chunk * each + 1 : (chunk + 1) * each]:
            total = total + ref[...].astype(jnp.float32)
        out[:, chunk * width : (chunk + 1) * width] = total


def total_of(parts, chunks):
    rows, width = parts[0].shape
    return pl.pallas_call(
        functools.partial(total_body, chunks),
        out_shape=jax.ShapeDtypeStruct((rows, width * chunks), jnp.float32),
        in_specs=[VMEM] * len(parts),
        out_specs=VMEM,
        name="total",
    )(*parts)


def shards(basis_values, occ_coef, listed_panels, centres, point_weights):
    width = occ_coef.shape[1]
    points = basis_values.shape[0]
    terms = lax.axis_size("coef")
    chunks = CHUNKS if width % (CHUNKS * LANES) == 0 else 1
    wide = width // chunks
    batch = lax.axis_index("grid")
    core = batch % 2
    first = (batch - core - REACH) * PANELS_DEV
    place = listed_panels[0] - first
    near_block, panel = place // PANELS_DEV, place % PANELS_DEV
    step, side = near_block // 2, near_block % 2
    edge = (step == 0) | (step == REACH)
    block = jnp.where(side == core, step, jnp.where(edge, 2 * REACH, REACH + step))
    table = jnp.stack([block, panel]).astype(jnp.int32)

    cut = [lax.slice_in_dim(occ_coef, c * wide, (c + 1) * wide, axis=1) for c in range(chunks)]
    distances = (4, 2, -2, -4)
    far = [{d: from_behind(cut[c], d) for d in (2, -2, 4, -4)} for c in range(chunks)]
    turned = basis_values.T
    fields = {}
    for c in range(chunks):
        got = far[c]
        mine = [got[4], got[2], cut[c], got[-2], got[-4]]
        edge_block = jnp.where(core == 0, got[-4], got[4])
        other = [core_swap(x) for x in (got[2], cut[c], got[-2], edge_block)]
        own = field_of(table, basis_values, mine + other)
        shifted = [coef_shift(own, t) for t in range(1, terms)]
        outer = outer_halo(own)
        fields[0, 0, c] = own
        fields[1, 0, c] = core_swap(own)
        fields[2, 0, c] = outer
        for t in range(1, terms):
            fields[0, t, c] = shifted[t - 1]
            fields[1, t, c] = core_swap(shifted[t - 1])
            fields[2, t, c] = coef_shift(outer, t)

    anchor = jnp.zeros((), jnp.int32)
    padded_centres = jnp.pad(centres, ((0, 0), (points, points)))
    outside = jnp.where(core == 0, batch - 1, batch + 1)
    of = lambda b: lax.dynamic_slice(padded_centres, (anchor, (b + 1) * points), (3, points))
    near_centres = jnp.concatenate([of(batch), of(batch + 1 - 2 * core), of(outside)], 1)
    flat = [
        fields[near, t, c] for near in range(3) for t in range(terms) for c in range(chunks)
    ]
    mixed = mixed_of(of(batch).T, near_centres, flat, terms, chunks)
    parts = []
    for c in range(chunks):
        stay, leave = tiles_of(
            table, mixed, fields[0, 0, c], fields[1, 0, c], fields[2, 0, c],
            point_weights[:, None], turned,
        )
        sums = paired_of(core.reshape(1).astype(jnp.int32), stay, core_swap(leave))
        parts.append(sums[REACH // 2])
        for i, distance in enumerate((-4, -2, 0, 2, 4)):
            if distance:
                parts.append(from_behind(sums[i], distance))
    return total_of(parts, chunks)


def solution(mesh):
    placed = (P("grid", None), P("grid", "coef"), P("grid", None), P(), P("grid"))
    return jax.shard_map(
        shards, mesh=mesh, in_specs=placed, out_specs=P("grid", "coef"), check_vma=False
    )
```

```python
import functools
import jax
import jax.numpy as jnp
from jax import lax
from jax.experimental import pallas as pl
from jax.experimental.pallas import tpu as pltpu
from jax.sharding import PartitionSpec as P

ORBITALS = 1024
PANEL_ROWS = 128
PANELS_DEV = 5
REACH = 4
LISTED = 21
CHUNKS = 2
SPLIT_IN = 384
SPLIT_OUT = 320
LANES = 128


OWN, SIDE, ALONG, AGAINST, DIAGONAL = KINDS = range(5)
LEAVING = (OWN, SIDE, ALONG, DIAGONAL)


def core_route():
    return [(i, i ^ 1) for i in range(lax.axis_size("grid"))]


def side_route():
    return [(i, i ^ 2) for i in range(lax.axis_size("grid"))]


def z_route(sign):
    count = lax.axis_size("grid")
    ends = [(i, i + (sign if i // 2 % 2 == 0 else -sign) * REACH) for i in range(count)]
    return [(i, j) for i, j in ends if 0 <= j < count]


def halo_route():
    return [pair for i in range(1, lax.axis_size("grid") - 1, 2) for pair in ((i, i + 1), (i + 1, i))]


def send(block, route):
    return lax.ppermute(block, "grid", route)


def coef_shift(block, shift):
    count = lax.axis_size("coef")
    return lax.ppermute(block, "coef", [(i, (i + shift) % count) for i in range(count)])


def add(a, b):
    return (a.astype(jnp.float32) + b.astype(jnp.float32)).astype(a.dtype)


VMEM = pl.BlockSpec(memory_space=pltpu.VMEM)


HBM = pl.BlockSpec(memory_space=pltpu.HBM)
SMEM = pl.BlockSpec(memory_space=pltpu.SMEM)
SPOTS = len(KINDS) * PANELS_DEV


def pack_body(*refs):
    blocks, out = refs[:-1], refs[-1]
    at = 0
    for ref in blocks:
        out[at : at + ref.shape[0], :] = ref[...]
        at += ref.shape[0]


def pack_of(blocks):
    rows = sum(block.shape[0] for block in blocks)
    return pl.pallas_call(
        pack_body,
        out_shape=jax.ShapeDtypeStruct((rows, blocks[0].shape[1]), blocks[0].dtype),
        in_specs=[VMEM] * len(blocks),
        out_specs=VMEM,
        compiler_params=pltpu.CompilerParams(vmem_limit_bytes=14 << 20),
        name="pack",
    )(*blocks)


def panel_rows(index):
    return pl.ds(pl.multiple_of(index * PANEL_ROWS, PANEL_ROWS), PANEL_ROWS)


def field_body(spans, chunks, slots, basis, *refs):
    count = len(refs) - 2 - chunks
    blocks, outs, sems = refs[:count], refs[count:-1], refs[-1]
    out, rest, chosen = outs[0], outs[1:chunks], outs[chunks:]
    targets = [chosen[0], *rest]
    wide = out.shape[1]
    for spot, (at, row) in enumerate(spans):
        slot = slots[0, spot]

        @pl.when(slot >= 0)
        def _():
            for c, target in enumerate(targets):
                source = blocks[at].at[pl.ds(row, PANEL_ROWS), pl.ds(c * wide, wide)]
                pltpu.make_async_copy(source, target.at[panel_rows(slot)], sems.at[c, slot]).start()

    def wait(c):
        for slot in range(LISTED):
            source = blocks[0].at[pl.ds(0, PANEL_ROWS), pl.ds(0, wide)]
            target = targets[c].at[pl.ds(slot * PANEL_ROWS, PANEL_ROWS)]
            pltpu.make_async_copy(source, target, sems.at[c, slot]).wait()

    wait(0)
    value = jnp.dot(basis[...], chosen[0][...], preferred_element_type=jnp.float32)
    out[...] = value.astype(out.dtype)
    for c in range(1, chunks):
        wait(c)


def field_of(slots, basis, blocks, spans, chunks):
    points, wide = basis.shape[0], blocks[0].shape[1] // chunks
    rest = jax.ShapeDtypeStruct((LISTED * PANEL_ROWS, wide), jnp.bfloat16)
    return pl.pallas_call(
        functools.partial(field_body, spans, chunks),
        out_shape=[jax.ShapeDtypeStruct((points, wide), jnp.bfloat16)] + [rest] * (chunks - 1),
        in_specs=[SMEM, VMEM] + [HBM] * len(blocks),
        out_specs=[VMEM] * chunks,
        scratch_shapes=[
            pltpu.VMEM((LISTED * PANEL_ROWS, wide), jnp.bfloat16),
            pltpu.SemaphoreType.DMA((chunks, LISTED)),
        ],
        cost_estimate=pl.CostEstimate(
            flops=2 * basis.size * wide, bytes_accessed=4 * basis.size, transcendentals=0
        ),
        compiler_params=pltpu.CompilerParams(vmem_limit_bytes=16 << 20),
        name="field",
    )(slots, basis, *[pltpu.with_memory_space_constraint(block, pltpu.HBM) for block in blocks])


def product_body(basis, chosen, out):
    value = jnp.dot(basis[...], chosen[...], preferred_element_type=jnp.float32)
    out[...] = value.astype(out.dtype)


def product_of(basis, chosen):
    return pl.pallas_call(
        product_body,
        out_shape=jax.ShapeDtypeStruct((basis.shape[0], chosen.shape[1]), jnp.bfloat16),
        in_specs=[VMEM, VMEM],
        out_specs=VMEM,
        cost_estimate=pl.CostEstimate(
            flops=2 * basis.size * chosen.shape[1], bytes_accessed=4 * basis.size, transcendentals=0
        ),
        compiler_params=pltpu.CompilerParams(vmem_limit_bytes=12 << 20),
        name="product",
    )(basis, chosen)


def mixed_body(terms, chunks, nears, rows, own_centres, near_centres, *refs):
    fields, out = refs[:-1], refs[-1]
    points = fields[0].shape[0]
    count = terms * chunks
    here = pl.ds(pl.multiple_of(pl.program_id(0) * rows, rows), rows)
    scale = 1.0 / float(ORBITALS) ** 0.5
    for near in range(nears):
        density = jnp.zeros((rows, points), jnp.float32)
        for term in range(terms):
            total = jnp.zeros((rows, points), jnp.float32)
            for at in range(term * chunks, (term + 1) * chunks):
                total = total + lax.dot_general(
                    fields[at][here, :],
                    fields[len(fields) - (nears - near) * count + at][...],
                    (((1,), (1,)), ((), ())),
                    preferred_element_type=jnp.float32,
                )
            density = density + (total * scale).astype(jnp.bfloat16).astype(jnp.float32)
        distance = jnp.zeros((rows, points), jnp.float32)
        for axis in range(3):
            gap = own_centres[here, axis : axis + 1] - near_centres[
                axis : axis + 1, near * points : (near + 1) * points
            ]
            distance = distance + gap * gap
        out[:, near * points : (near + 1) * points] = (
            lax.rsqrt(distance + 0.25) * density
        ).astype(out.dtype)


def mixed_of(own_centres, near_centres, fields, terms, chunks):
    points = own_centres.shape[0]
    nears = near_centres.shape[1] // points
    rows = points // 2 if points % 32 == 0 else points
    width = fields[0].shape[1]
    return pl.pallas_call(
        functools.partial(mixed_body, terms, chunks, nears, rows),
        grid=(points // rows,),
        out_shape=jax.ShapeDtypeStruct((points, nears * points), jnp.bfloat16),
        in_specs=[VMEM] * (2 + len(fields)),
        out_specs=pl.BlockSpec((rows, nears * points), lambda i: (i, 0)),
        cost_estimate=pl.CostEstimate(
            flops=2 * nears * points * points * width * chunks * terms,
            bytes_accessed=6 * nears * points * points,
            transcendentals=nears * points * points,
        ),
        compiler_params=pltpu.CompilerParams(vmem_limit_bytes=16 << 20),
        name="mixed",
    )(own_centres, near_centres, *fields)


def tiles_body(chunks, slots, mixed, mixed_outer, weights, basis, *refs):
    fields, (tiles, leave) = refs[:-2], refs[-2:]
    points, _ = fields[0].shape
    parts = []
    for c in range(chunks):
        own, swapped, outer = fields[c], fields[chunks + c], fields[2 * chunks + c]
        exchanged = jnp.dot(mixed[:, :points], own[...], preferred_element_type=jnp.float32)
        exchanged += jnp.dot(mixed[:, points:], swapped[...], preferred_element_type=jnp.float32)
        exchanged += jnp.dot(mixed_outer[...], outer[...], preferred_element_type=jnp.float32)
        parts.append(
            (exchanged * weights[...] * (1.0 / float(3 * points) ** 0.5)).astype(jnp.bfloat16)
        )
    weighted = jnp.concatenate(parts, 1)
    product = lax.dot_general(
        basis[...], weighted, (((0,), (0,)), ((), ())), preferred_element_type=jnp.float32
    )
    tiles[...] = (product * (1.0 / float(points) ** 0.5)).astype(tiles.dtype)
    for kind in LEAVING:
        for panel in range(PANELS_DEV):
            slot = slots[0, SPOTS + kind * PANELS_DEV + panel]
            if kind == ALONG:
                slot = jnp.maximum(slot, slots[0, SPOTS + AGAINST * PANELS_DEV + panel])
            at = (LEAVING.index(kind) * PANELS_DEV + panel) * PANEL_ROWS
            rows = slice(at, at + PANEL_ROWS)

            @pl.when(slot >= 0)
            def _():
                leave[rows, :] = tiles[panel_rows(slot), :]

            @pl.when(slot < 0)
            def _():
                leave[rows, :] = jnp.zeros((PANEL_ROWS, leave.shape[1]), leave.dtype)


def tiles_of(slots, mixed, mixed_outer, weights, basis, fields, chunks):
    width = fields[0].shape[1] * chunks
    block = PANELS_DEV * PANEL_ROWS
    return pl.pallas_call(
        functools.partial(tiles_body, chunks),
        out_shape=(
            jax.ShapeDtypeStruct((LISTED * PANEL_ROWS, width), jnp.bfloat16),
            jax.ShapeDtypeStruct((len(LEAVING) * block, width), jnp.bfloat16),
        ),
        in_specs=[pl.BlockSpec(memory_space=pltpu.SMEM)] + [VMEM] * (4 + len(fields)),
        out_specs=(VMEM, VMEM),
        cost_estimate=pl.CostEstimate(
            flops=2 * (mixed.size + mixed_outer.size + basis.size) * width,
            bytes_accessed=4 * basis.size,
            transcendentals=0,
        ),
        compiler_params=pltpu.CompilerParams(vmem_limit_bytes=30 << 20),
        name="tiles",
    )(slots, mixed, mixed_outer, weights, basis, *fields)


def paired_body(parity, slots, tiles, came, own, side_a, side_b, along, against_a, against_b, diag_a, diag_b):
    core, column = parity[0], parity[1]
    outs = {
        OWN: [own], SIDE: [side_a, side_b], ALONG: [along],
        AGAINST: [against_a, against_b], DIAGONAL: [diag_a, diag_b],
    }
    for kind in KINDS:
        other = LEAVING.index(ALONG if kind == AGAINST else kind)
        for panel in range(PANELS_DEV):
            slot = slots[0, kind * PANELS_DEV + panel]
            tile = tiles[panel_rows(jnp.maximum(slot, 0)), :].astype(jnp.float32)
            tile = jnp.where(slot >= 0, tile, 0.0)
            at = (other * PANELS_DEV + panel) * PANEL_ROWS
            extra = came[at : at + PANEL_ROWS, :].astype(jnp.float32)
            if kind in (ALONG, AGAINST):
                mine = core == column if kind == AGAINST else core != column
                extra = jnp.where(mine, extra, 0.0)
            total = tile + extra
            first = 0
            for out in outs[kind]:
                low = max(panel * PANEL_ROWS, first)
                high = min((panel + 1) * PANEL_ROWS, first + out.shape[0])
                if low < high:
                    base = panel * PANEL_ROWS
                    out[low - first : high - first, :] = total[low - base : high - base].astype(out.dtype)
                first += out.shape[0]


def paired_of(parity, slots, tiles, came):
    block, width = PANELS_DEV * PANEL_ROWS, tiles.shape[1]
    shapes = [jax.ShapeDtypeStruct((block, width), jnp.float32)]
    for rows in (SPLIT_OUT, block - SPLIT_OUT, block) + (SPLIT_OUT, block - SPLIT_OUT) * 2:
        shapes.append(jax.ShapeDtypeStruct((rows, width), jnp.bfloat16))
    return pl.pallas_call(
        paired_body,
        out_shape=tuple(shapes),
        in_specs=[SMEM, SMEM, VMEM, VMEM],
        out_specs=(VMEM,) * len(shapes),
        cost_estimate=pl.CostEstimate(
            flops=2 * tiles.size, bytes_accessed=6 * tiles.size, transcendentals=0
        ),
        compiler_params=pltpu.CompilerParams(vmem_limit_bytes=20 << 20),
        name="paired",
    )(parity, slots, tiles, came)


def total_body(own, side_a, side_b, along, against_a, against_b, out):
    rows = side_a.shape[0]
    wide = lambda ref: ref[...].astype(jnp.float32)
    out[:rows, :] = own[:rows, :] + wide(side_a) + along[:rows, :].astype(jnp.float32) + wide(against_a)
    out[rows:, :] = own[rows:, :] + wide(side_b) + along[rows:, :].astype(jnp.float32) + wide(against_b)


def total_of(parts):
    return pl.pallas_call(
        total_body,
        out_shape=jax.ShapeDtypeStruct(parts[0].shape, jnp.float32),
        in_specs=[VMEM] * len(parts),
        out_specs=VMEM,
        compiler_params=pltpu.CompilerParams(vmem_limit_bytes=8 << 20),
        name="total",
    )(*parts)


def tiled(basis_values, occ_coef, listed_panels, centres, point_weights):
    width = occ_coef.shape[1]
    points = basis_values.shape[0]
    terms = lax.axis_size("coef")
    chunks = CHUNKS if width % (CHUNKS * LANES) == 0 else 1
    batch = lax.axis_index("grid")
    core = batch % 2
    column = batch // 2 % 2
    first = (batch - core - REACH) * PANELS_DEV
    place = listed_panels[0] - first
    near_block, panel = place // PANELS_DEV, place % PANELS_DEV
    step, side = near_block // 2 - REACH // 2, near_block % 2
    toward = jnp.where(column == 0, step, -step)
    kind = jnp.where(
        toward == 0, OWN, jnp.where(toward == 1, SIDE, jnp.where(toward == -1, DIAGONAL,
        jnp.where(toward == 2, AGAINST, ALONG))))
    found = jnp.where(side == core, 0, SPOTS) + kind * PANELS_DEV + panel
    spots = jnp.arange(2 * SPOTS, dtype=jnp.int32)
    order = jnp.arange(LISTED, dtype=jnp.int32)
    slots = jnp.max(
        jnp.where(found[:, None] == spots[None, :], order[:, None], -1), axis=0, keepdims=True
    )
    parity = jnp.stack([core, column]).astype(jnp.int32)

    side_ = send(occ_coef, side_route())
    along = send(occ_coef, z_route(1))
    against = send(occ_coef, z_route(-1))
    relay_a = send(side_[:SPLIT_IN], z_route(1))
    relay_b = send(against[SPLIT_IN:], side_route())
    swapped = send(pack_of([occ_coef, side_, along, against]), core_route())
    late_a = send(relay_a, core_route())
    late_b = send(relay_b, core_route())
    blocks = [occ_coef, side_, along, against, relay_a, relay_b, swapped, late_a, late_b]
    spans = []
    for at, late in ((0, 4), (6, 7)):
        for kind_ in KINDS:
            for panel_ in range(PANELS_DEV):
                row = panel_ * PANEL_ROWS
                if kind_ == DIAGONAL:
                    spans.append((late, row) if row < SPLIT_IN else (late + 1, row - SPLIT_IN))
                elif at:
                    spans.append((at, kind_ * PANELS_DEV * PANEL_ROWS + row))
                else:
                    spans.append((kind_, row))
    chosen = field_of(slots, basis_values, blocks, spans, chunks)
    fields = {}
    for c in range(chunks):
        own = product_of(basis_values, chosen[c]) if c else chosen[0]
        fields[0, 0, c] = own
        shifted = [coef_shift(own, t) for t in range(1, terms)]
        fields[2, 0, c] = send(own, halo_route())
        fields[1, 0, c] = send(own, core_route())
        for t in range(1, terms):
            fields[0, t, c] = shifted[t - 1]
            fields[1, t, c] = send(shifted[t - 1], core_route())
            if c % 2 == 0:
                fields[2, t, c] = coef_shift(fields[2, 0, c], t)
            else:
                fields[2, t, c] = send(shifted[t - 1], halo_route())

    anchor = jnp.zeros((), jnp.int32)
    padded_centres = jnp.pad(centres, ((0, 0), (points, points)))
    outside = jnp.where(core == 0, batch - 1, batch + 1)
    of = lambda b: lax.dynamic_slice(padded_centres, (anchor, (b + 1) * points), (3, points))
    near_centres = jnp.concatenate([of(batch), of(batch + 1 - 2 * core)], 1)
    own_centres = of(batch).T
    flat = [
        [fields[near, t, c] for t in range(terms) for c in range(chunks)] for near in range(3)
    ]
    mixed = mixed_of(own_centres, near_centres, flat[0] + flat[1], terms, chunks)
    mixed_outer = mixed_of(own_centres, of(outside), flat[0] + flat[2], terms, chunks)
    tiles, leave = tiles_of(
        slots, mixed, mixed_outer, point_weights[:, None], basis_values,
        [fields[near, 0, c] for near in range(3) for c in range(chunks)], chunks,
    )
    came = send(leave, core_route())
    own, side_a, side_b, along, against_a, against_b, diag_a, diag_b = paired_of(parity, slots, tiles, came)
    moved_b = send(diag_b, side_route())
    moved_a = send(diag_a, z_route(-1))
    home = [
        own,
        send(add(side_a, moved_a), side_route()),
        send(side_b, side_route()),
        send(along, z_route(-1)),
        send(against_a, z_route(1)),
        send(add(against_b, moved_b), z_route(1)),
    ]
    return total_of(home)


def solution(mesh):
    placed = (P("grid", None), P("grid", "coef"), P("grid", None), P(), P("grid"))
    return jax.shard_map(tiled, mesh=mesh, in_specs=placed, out_specs=P("grid", "coef"), check_vma=False)
```

```python
import functools
import jax
import jax.numpy as jnp
from jax import lax
from jax.experimental import pallas as pl
from jax.experimental.pallas import tpu as pltpu
from jax.sharding import PartitionSpec as P

ORBITALS = 1024
PANEL_ROWS = 128
PANELS_DEV = 5
REACH = 4
LISTED = 21
CHUNKS = 2
SPLIT_IN = 384
SPLIT_OUT = 288
LANES = 128


OWN, SIDE, ALONG, AGAINST, DIAGONAL = KINDS = range(5)
LEAVING = (OWN, SIDE, ALONG, DIAGONAL)


def core_route():
    return [(i, i ^ 1) for i in range(lax.axis_size("grid"))]


def side_route():
    return [(i, i ^ 2) for i in range(lax.axis_size("grid"))]


def z_route(sign):
    count = lax.axis_size("grid")
    ends = [(i, i + (sign if i // 2 % 2 == 0 else -sign) * REACH) for i in range(count)]
    return [(i, j) for i, j in ends if 0 <= j < count]


def halo_route():
    return [pair for i in range(1, lax.axis_size("grid") - 1, 2) for pair in ((i, i + 1), (i + 1, i))]


def send(block, route):
    return lax.ppermute(block, "grid", route)


def coef_shift(block, shift):
    count = lax.axis_size("coef")
    return lax.ppermute(block, "coef", [(i, (i + shift) % count) for i in range(count)])


def add(a, b):
    return (a.astype(jnp.float32) + b.astype(jnp.float32)).astype(a.dtype)


VMEM = pl.BlockSpec(memory_space=pltpu.VMEM)


HBM = pl.BlockSpec(memory_space=pltpu.HBM)
SMEM = pl.BlockSpec(memory_space=pltpu.SMEM)
SPOTS = len(KINDS) * PANELS_DEV


def cut_body(block, top, bottom):
    rows = top.shape[0]
    top[...] = block[:rows, :]
    bottom[...] = block[rows:, :]


def cut_of(block):
    rows, width = block.shape
    shapes = [jax.ShapeDtypeStruct((n, width), block.dtype) for n in (SPLIT_IN, rows - SPLIT_IN)]
    return pl.pallas_call(
        cut_body,
        out_shape=tuple(shapes),
        in_specs=[VMEM],
        out_specs=(VMEM, VMEM),
        compiler_params=pltpu.CompilerParams(vmem_limit_bytes=4 << 20),
        name="cut",
    )(block)


def load_body(source, target, sem):
    copy = pltpu.make_async_copy(source, target, sem)
    copy.start()
    copy.wait()


def load_of(block):
    return pl.pallas_call(
        load_body,
        out_shape=jax.ShapeDtypeStruct(block.shape, block.dtype),
        in_specs=[HBM],
        out_specs=VMEM,
        scratch_shapes=[pltpu.SemaphoreType.DMA(())],
        compiler_params=pltpu.CompilerParams(vmem_limit_bytes=8 << 20),
        name="load",
    )(pltpu.with_memory_space_constraint(block, pltpu.HBM))


def panel_rows(index):
    return pl.ds(pl.multiple_of(index * PANEL_ROWS, PANEL_ROWS), PANEL_ROWS)


def field_body(spans, slots, basis, *refs):
    blocks, (out, chosen, sems) = refs[:-3], refs[-3:]
    wide = out.shape[1]
    for spot, (at, row) in enumerate(spans):
        slot = slots[0, spot]

        @pl.when(slot >= 0)
        def _():
            source = blocks[at].at[pl.ds(row, PANEL_ROWS)]
            pltpu.make_async_copy(source, chosen.at[panel_rows(slot)], sems.at[slot]).start()

    for slot in range(LISTED):
        target = chosen.at[pl.ds(slot * PANEL_ROWS, PANEL_ROWS)]
        pltpu.make_async_copy(blocks[0].at[pl.ds(0, PANEL_ROWS)], target, sems.at[slot]).wait()
    value = jnp.dot(basis[...], chosen[:, :wide], preferred_element_type=jnp.float32)
    out[...] = value.astype(out.dtype)


def field_of(slots, basis, blocks, spans, chunks):
    points, width = basis.shape[0], blocks[0].shape[1]
    return pl.pallas_call(
        functools.partial(field_body, spans),
        out_shape=(
            jax.ShapeDtypeStruct((points, width // chunks), jnp.bfloat16),
            jax.ShapeDtypeStruct((LISTED * PANEL_ROWS, width), jnp.bfloat16),
        ),
        in_specs=[SMEM, VMEM] + [HBM] * len(blocks),
        out_specs=(VMEM, VMEM),
        scratch_shapes=[pltpu.SemaphoreType.DMA((LISTED,))],
        cost_estimate=pl.CostEstimate(
            flops=2 * basis.size * width, bytes_accessed=4 * basis.size, transcendentals=0
        ),
        compiler_params=pltpu.CompilerParams(vmem_limit_bytes=16 << 20),
        name="field",
    )(slots, basis, *[pltpu.with_memory_space_constraint(x, pltpu.HBM) for x in blocks])


def product_body(start, basis, chosen, out):
    value = jnp.dot(
        basis[...], chosen[:, start : start + out.shape[1]], preferred_element_type=jnp.float32
    )
    out[...] = value.astype(out.dtype)


def product_of(basis, chosen, start, wide):
    return pl.pallas_call(
        functools.partial(product_body, start),
        out_shape=jax.ShapeDtypeStruct((basis.shape[0], wide), jnp.bfloat16),
        in_specs=[VMEM, VMEM],
        out_specs=VMEM,
        cost_estimate=pl.CostEstimate(
            flops=2 * basis.size * wide, bytes_accessed=4 * basis.size, transcendentals=0
        ),
        compiler_params=pltpu.CompilerParams(vmem_limit_bytes=14 << 20),
        name="product",
    )(basis, chosen)


def mixed_body(terms, chunks, nears, rows, own_centres, near_centres, *refs):
    fields, out, turned = refs[:-2], refs[-2], refs[-1]
    points = fields[0].shape[0]
    count = terms * chunks

    @pl.when(pl.program_id(0) == 0)
    def _():
        turned[...] = own_centres[...].T

    here = pl.ds(pl.multiple_of(pl.program_id(0) * rows, rows), rows)
    scale = 1.0 / float(ORBITALS) ** 0.5
    for near in range(nears):
        density = jnp.zeros((rows, points), jnp.float32)
        for term in range(terms):
            total = jnp.zeros((rows, points), jnp.float32)
            for at in range(term * chunks, (term + 1) * chunks):
                total = total + lax.dot_general(
                    fields[at][here, :],
                    fields[len(fields) - (nears - near) * count + at][...],
                    (((1,), (1,)), ((), ())),
                    preferred_element_type=jnp.float32,
                )
            density = density + (total * scale).astype(jnp.bfloat16).astype(jnp.float32)
        distance = jnp.zeros((rows, points), jnp.float32)
        for axis in range(3):
            gap = turned[here, axis : axis + 1] - near_centres[
                axis : axis + 1, near * points : (near + 1) * points
            ]
            distance = distance + gap * gap
        out[:, near * points : (near + 1) * points] = (
            lax.rsqrt(distance + 0.25) * density
        ).astype(out.dtype)


def mixed_of(own_centres, near_centres, fields, terms, chunks):
    points = own_centres.shape[1]
    nears = near_centres.shape[1] // points
    rows = points // 2 if points % 32 == 0 else points
    width = fields[0].shape[1]
    return pl.pallas_call(
        functools.partial(mixed_body, terms, chunks, nears, rows),
        grid=(points // rows,),
        out_shape=jax.ShapeDtypeStruct((points, nears * points), jnp.bfloat16),
        in_specs=[VMEM] * (2 + len(fields)),
        out_specs=pl.BlockSpec((rows, nears * points), lambda i: (i, 0)),
        scratch_shapes=[pltpu.VMEM((points, own_centres.shape[0]), jnp.float32)],
        cost_estimate=pl.CostEstimate(
            flops=2 * nears * points * points * width * chunks * terms,
            bytes_accessed=6 * nears * points * points,
            transcendentals=nears * points * points,
        ),
        compiler_params=pltpu.CompilerParams(vmem_limit_bytes=16 << 20),
        name="mixed",
    )(own_centres, near_centres, *fields)


def tiles_body(slots, mixed, mixed_outer, weights, basis, own, swapped, outer, tiles, leave):
    points = own.shape[0]
    exchanged = jnp.dot(mixed[:, :points], own[...], preferred_element_type=jnp.float32)
    exchanged += jnp.dot(mixed[:, points:], swapped[...], preferred_element_type=jnp.float32)
    exchanged += jnp.dot(mixed_outer[...], outer[...], preferred_element_type=jnp.float32)
    weighted = (exchanged * weights[...] * (1.0 / float(3 * points) ** 0.5)).astype(jnp.bfloat16)
    product = lax.dot_general(
        basis[...], weighted, (((0,), (0,)), ((), ())), preferred_element_type=jnp.float32
    )
    tiles[...] = (product * (1.0 / float(points) ** 0.5)).astype(tiles.dtype)
    for kind in LEAVING:
        for panel in range(PANELS_DEV):
            slot = slots[0, SPOTS + kind * PANELS_DEV + panel]
            if kind == ALONG:
                slot = jnp.maximum(slot, slots[0, SPOTS + AGAINST * PANELS_DEV + panel])
            at = (LEAVING.index(kind) * PANELS_DEV + panel) * PANEL_ROWS
            rows = slice(at, at + PANEL_ROWS)

            @pl.when(slot >= 0)
            def _():
                leave[rows, :] = tiles[panel_rows(slot), :]

            @pl.when(slot < 0)
            def _():
                leave[rows, :] = jnp.zeros((PANEL_ROWS, leave.shape[1]), leave.dtype)


def tiles_of(slots, mixed, mixed_outer, weights, basis, fields):
    width = fields[0].shape[1]
    block = PANELS_DEV * PANEL_ROWS
    return pl.pallas_call(
        tiles_body,
        out_shape=(
            jax.ShapeDtypeStruct((LISTED * PANEL_ROWS, width), jnp.bfloat16),
            jax.ShapeDtypeStruct((len(LEAVING) * block, width), jnp.bfloat16),
        ),
        in_specs=[pl.BlockSpec(memory_space=pltpu.SMEM)] + [VMEM] * (4 + len(fields)),
        out_specs=(VMEM, VMEM),
        cost_estimate=pl.CostEstimate(
            flops=2 * (mixed.size + mixed_outer.size + basis.size) * width,
            bytes_accessed=4 * basis.size,
            transcendentals=0,
        ),
        compiler_params=pltpu.CompilerParams(vmem_limit_bytes=20 << 20),
        name="tiles",
    )(slots, mixed, mixed_outer, weights, basis, *fields)


def paired_body(chunks, parity, slots, *refs):
    for c in range(chunks):
        paired_columns(c, parity, slots, refs[c], refs[chunks + c], *refs[2 * chunks :])


def paired_columns(
    c, parity, slots, tiles, came, own, side_a, side_b, along, against_a, against_b, diag_a, diag_b
):
    columns = slice(c * tiles.shape[1], (c + 1) * tiles.shape[1])
    core, column = parity[0], parity[1]
    outs = {
        OWN: [own], SIDE: [side_a, side_b], ALONG: [along],
        AGAINST: [against_a, against_b], DIAGONAL: [diag_a, diag_b],
    }
    for kind in KINDS:
        other = LEAVING.index(ALONG if kind == AGAINST else kind)
        for panel in range(PANELS_DEV):
            slot = slots[0, kind * PANELS_DEV + panel]
            tile = tiles[panel_rows(jnp.maximum(slot, 0)), :].astype(jnp.float32)
            tile = jnp.where(slot >= 0, tile, 0.0)
            at = (other * PANELS_DEV + panel) * PANEL_ROWS
            extra = came[at : at + PANEL_ROWS, :].astype(jnp.float32)
            if kind in (ALONG, AGAINST):
                mine = core == column if kind == AGAINST else core != column
                extra = jnp.where(mine, extra, 0.0)
            total = tile + extra
            first = 0
            for out in outs[kind]:
                low = max(panel * PANEL_ROWS, first)
                high = min((panel + 1) * PANEL_ROWS, first + out.shape[0])
                if low < high:
                    base = panel * PANEL_ROWS
                    piece = total[low - base : high - base].astype(out.dtype)
                    out[low - first : high - first, columns] = piece
                first += out.shape[0]


def paired_of(parity, slots, tiles, came):
    chunks = len(tiles)
    block, width = PANELS_DEV * PANEL_ROWS, tiles[0].shape[1] * chunks
    shapes = [jax.ShapeDtypeStruct((block, width), jnp.float32)]
    for rows in (SPLIT_OUT, block - SPLIT_OUT, block) + (SPLIT_OUT, block - SPLIT_OUT) * 2:
        shapes.append(jax.ShapeDtypeStruct((rows, width), jnp.bfloat16))
    return pl.pallas_call(
        functools.partial(paired_body, chunks),
        out_shape=tuple(shapes),
        in_specs=[SMEM, SMEM] + [VMEM] * (2 * chunks),
        out_specs=(VMEM,) * len(shapes),
        cost_estimate=pl.CostEstimate(
            flops=2 * LISTED * PANEL_ROWS * width, bytes_accessed=8 * block * width, transcendentals=0
        ),
        compiler_params=pltpu.CompilerParams(vmem_limit_bytes=20 << 20),
        name="paired",
    )(parity, slots, *tiles, *came)


def total_body(own, side_a, side_b, along, against_a, against_b, out):
    rows = side_a.shape[0]
    wide = lambda ref: ref[...].astype(jnp.float32)
    out[:rows, :] = own[:rows, :] + wide(side_a) + along[:rows, :].astype(jnp.float32) + wide(against_a)
    out[rows:, :] = own[rows:, :] + wide(side_b) + along[rows:, :].astype(jnp.float32) + wide(against_b)


def total_of(parts):
    return pl.pallas_call(
        total_body,
        out_shape=jax.ShapeDtypeStruct(parts[0].shape, jnp.float32),
        in_specs=[VMEM] * len(parts),
        out_specs=VMEM,
        compiler_params=pltpu.CompilerParams(vmem_limit_bytes=8 << 20),
        name="total",
    )(*parts)


def tiled(basis_values, occ_coef, listed_panels, centres, point_weights):
    width = occ_coef.shape[1]
    points = basis_values.shape[0]
    terms = lax.axis_size("coef")
    chunks = CHUNKS if width % (CHUNKS * LANES) == 0 else 1
    wide = width // chunks
    batch = lax.axis_index("grid")
    core = batch % 2
    column = batch // 2 % 2
    first = (batch - core - REACH) * PANELS_DEV
    place = listed_panels[0] - first
    near_block, panel = place // PANELS_DEV, place % PANELS_DEV
    step, side = near_block // 2 - REACH // 2, near_block % 2
    toward = jnp.where(column == 0, step, -step)
    kind = jnp.where(
        toward == 0, OWN, jnp.where(toward == 1, SIDE, jnp.where(toward == -1, DIAGONAL,
        jnp.where(toward == 2, AGAINST, ALONG))))
    found = jnp.where(side == core, 0, SPOTS) + kind * PANELS_DEV + panel
    spots = jnp.arange(2 * SPOTS, dtype=jnp.int32)
    order = jnp.arange(LISTED, dtype=jnp.int32)
    slots = jnp.max(
        jnp.where(found[:, None] == spots[None, :], order[:, None], -1), axis=0, keepdims=True
    )
    parity = jnp.stack([core, column]).astype(jnp.int32)

    top, bottom = cut_of(occ_coef)
    near_basis = load_of(basis_values)
    along = send(occ_coef, z_route(1))
    side_top = send(top, side_route())
    side_bottom = send(bottom, side_route())
    against_top = send(top, z_route(-1))
    against_bottom = send(bottom, z_route(-1))
    relay_a = send(side_top, z_route(1))
    relay_b = send(against_bottom, side_route())
    held = [occ_coef, side_top, side_bottom, along, against_top, against_bottom, relay_a, relay_b]
    blocks = held + [send(block, core_route()) for block in held]
    first_of = {OWN: 0, SIDE: 1, ALONG: 3, AGAINST: 4, DIAGONAL: 6}
    spans = []
    for base in (0, len(held)):
        for kind_ in KINDS:
            for panel_ in range(PANELS_DEV):
                at, row = base + first_of[kind_], panel_ * PANEL_ROWS
                if kind_ not in (OWN, ALONG) and row >= SPLIT_IN:
                    at, row = at + 1, row - SPLIT_IN
                spans.append((at, row))
    opening, chosen = field_of(slots, near_basis, blocks, spans, chunks)
    fields = {}
    for c in range(chunks):
        own = product_of(near_basis, chosen, c * wide, wide) if c else opening
        fields[0, 0, c] = own
        shifted = [coef_shift(own, t) for t in range(1, terms)]
        fields[2, 0, c] = send(own, halo_route())
        fields[1, 0, c] = send(own, core_route())
        for t in range(1, terms):
            fields[0, t, c] = shifted[t - 1]
            fields[1, t, c] = send(shifted[t - 1], core_route())
            if c % 2 == 1:
                fields[2, t, c] = coef_shift(fields[2, 0, c], t)
            else:
                fields[2, t, c] = send(shifted[t - 1], halo_route())

    anchor = jnp.zeros((), jnp.int32)
    padded_centres = jnp.pad(centres, ((0, 5), (points, points)))
    outside = jnp.where(core == 0, batch - 1, batch + 1)
    of = lambda b: lax.dynamic_slice(padded_centres, (anchor, (b + 1) * points), (8, points))
    own_centres = of(batch)
    near_centres = jnp.concatenate([own_centres, of(batch + 1 - 2 * core)], 1)
    outer_centres = of(outside)
    flat = [
        [fields[near, t, c] for t in range(terms) for c in range(chunks)] for near in range(3)
    ]
    mixed = mixed_of(own_centres, near_centres, flat[0] + flat[1], terms, chunks)
    mixed_outer = mixed_of(own_centres, outer_centres, flat[0] + flat[2], terms, chunks)
    tiles, came = [], []
    for c in range(chunks):
        part, leave = tiles_of(
            slots, mixed, mixed_outer, point_weights[:, None], near_basis,
            [fields[near, 0, c] for near in range(3)],
        )
        tiles.append(part)
        came.append(send(leave, core_route()))
    own, side_a, side_b, along, against_a, against_b, diag_a, diag_b = paired_of(
        parity, slots, tiles, came
    )
    moved_b = send(diag_b, side_route())
    moved_a = send(diag_a, z_route(-1))
    home = [
        own,
        send(add(side_a, moved_a), side_route()),
        send(side_b, side_route()),
        send(along, z_route(-1)),
        send(against_a, z_route(1)),
        send(add(against_b, moved_b), z_route(1)),
    ]
    return total_of(home)


def solution(mesh):
    placed = (P("grid", None), P("grid", "coef"), P("grid", None), P(), P("grid"))
    return jax.shard_map(
        tiled, mesh=mesh, in_specs=placed, out_specs=P("grid", "coef"), check_vma=False
    )
```
